32 devices in a mesh: gx: 4 (over y, x), gy: 8 (over z, core).
Axes of the slice: x: 2, y: 2, z: 4, core: 2. Of those that a mesh axis runs over, the one named last changes fastest.
Arguments:
- positions: float32 [3, 262144], P(None, ('gx', 'gy')), may hold values from -6 to 6
- velocities: float32 [3, 262144], P(None, ('gx', 'gy')), may hold values from -4 to 4
- masses: float32 [262144], P(('gx', 'gy')), may hold values from 0.005 to 0.05
- long_kick: float32 [3, 262144], P(None, ('gx', 'gy')), may hold values from -3 to 3
- leaf_lists: int32 [8, 2048], P(None, ('gx', 'gy')), may hold values from 0 to 135, as said below
- ghost_ids: int32 [256], P(('gx', 'gy')), may hold values from 0 to 63, as said below
- leaf_counts: int32 [32], P(('gx', 'gy')), may hold values from 1 to 64, as said below
Outputs:
- new_positions: float32 [3, 262144], P(None, ('gx', 'gy'))
- new_velocities: float32 [3, 262144], P(None, ('gx', 'gy'))
The draws below stay inside these ranges and needn't reach their ends.
Inputs may be any that keep to these rules, and one draw needn't show every extreme that they name: leaf_counts of a domain is at least 1; the counts of domains (i, j) and (i, j + 4) for j below 4 sum to at most 80, and some pair reaches it with one count equal to 64. `leaf_lists`: every entry below 64 is below the count of its domain; entries from 64 on name pool ghost leaves. `ghost_ids`: each id is below the count of its domain; ids may repeat.
All inputs are finite; a program needn't handle non-finite values.
Results may differ from the reference program's by a relative error of at most 0.00011.
Values sent between devices are 32-bit elements; how exact they have to be, the bound alone decides.
A program may use at most 64 MiB of HBM per device.

```python
import math
import jax
import jax.numpy as jnp
from jax import lax

LEAF = 128
NEIGHBOURS = 8
LEAVES = 64
GHOSTS = 8
SUBCYCLES = 4
BAL = 40
SLABS = 4
COLUMNS = 8
DOMAINS = 32
PARTICLES = 262144


def pair_counts(key):
    base = jax.random.fold_in(key, 7)
    first_key, second_key = jax.random.split(base)
    half = COLUMNS // 2
    totals = jax.random.randint(first_key, (SLABS, half), 4, 2 * BAL + 1)
    totals = totals.at[0, 0].set(2 * BAL)
    lowest = jnp.maximum(1, totals - LEAVES)
    highest = jnp.minimum(LEAVES, totals - 1)
    first = jax.random.randint(second_key, (SLABS, half), lowest, highest + 1)
    first = first.at[0, 0].set(LEAVES)
    second = totals - first
    return jnp.concatenate([first, second], axis=1).reshape(-1).astype(jnp.int32)


def draw_leaf_counts(key, part):
    return pair_counts(key)


def draw_leaf_lists(key, part):
    counts = pair_counts(key)
    per_leaf = jnp.repeat(counts, LEAVES, total_repeat_length=DOMAINS * LEAVES)
    base = jax.random.fold_in(key, 11)
    own_key, ghost_key, pick_key = jax.random.split(base, 3)
    shape = (NEIGHBOURS, DOMAINS * LEAVES)
    own_pick = jax.random.randint(own_key, shape, 0, jnp.broadcast_to(per_leaf[None, :], shape))
    ghost_pick = LEAVES + jax.random.randint(ghost_key, shape, 0, 9 * GHOSTS)
    which = jax.random.randint(pick_key, shape, 0, 2)
    return jnp.where(which == 1, ghost_pick, own_pick).astype(jnp.int32)


def draw_ghost_ids(key, part):
    counts = pair_counts(key)
    per_ghost = jnp.repeat(counts, GHOSTS, total_repeat_length=DOMAINS * GHOSTS)
    base = jax.random.fold_in(key, 13)
    return jax.random.randint(base, (DOMAINS * GHOSTS,), 0, per_ghost).astype(jnp.int32)


def levels(key, shape, cuts, low, largest):
    def one(dim, blocks):
        steps = jax.random.uniform(jax.random.fold_in(jax.random.fold_in(key, 6), dim), (blocks,), jnp.float32, low / len(cuts), largest / len(cuts))
        return jnp.repeat(jnp.exp(steps), shape[dim] // blocks).reshape((-1,) + (1,) * (len(shape) - dim - 1))

    gain = one(*cuts[0])
    for cut in cuts[1:]:
        gain = gain * one(*cut)
    return gain


def scatter_about(rng, extent, deviation, limit, cuts=(), held_as=jnp.bfloat16):
    level = levels(rng, extent, cuts, -0.22, 0.18) if cuts else 1.0
    result = jax.random.normal(rng, extent, jnp.float32) * deviation * level
    return jnp.minimum(jnp.maximum(result, -limit), limit).astype(held_as)


def setup_inputs(seed: int = 0) -> dict:
    key_list = jax.random.split(jax.random.key(seed), 8)
    return {
        "positions": scatter_about(key_list[0], (3, PARTICLES), 1.0, 6.0, ((1, 32),), jnp.float32),
        "velocities": scatter_about(key_list[1], (3, PARTICLES), 0.5, 4.0, ((1, 32),), jnp.float32),
        "masses": jnp.clip(jnp.exp(math.log(0.05) - 2.3025851 * jax.random.uniform(key_list[2], (PARTICLES,), jnp.float32) ** levels(key_list[2], (PARTICLES,), ((0, 32),), -0.2, 0.2)), 0.005, 0.05),
        "long_kick": scatter_about(key_list[3], (3, PARTICLES), 0.3, 3.0, ((1, 32),), jnp.float32),
        "leaf_lists": draw_leaf_lists(jax.random.fold_in(key_list[7], 71), 0),
        "ghost_ids": draw_ghost_ids(jax.random.fold_in(key_list[7], 71), 0),
        "leaf_counts": draw_leaf_counts(jax.random.fold_in(key_list[7], 71), 0),
    }


soften_sq = 0.04
cutoff_sq = 9.0
time_step = 0.5

def pair_accel(targets, sources):
    offsets = sources[:3, :, None, :] - targets[:, :, :, None]
    distance = lax.optimization_barrier(jnp.sum(offsets * offsets, axis=0))
    tapers = jnp.square(jnp.maximum(1.0 - distance / cutoff_sq, 0.0))
    inverse = lax.rsqrt(distance + soften_sq)
    weight = sources[3][:, None, :] * tapers * inverse * inverse * inverse
    return lax.optimization_barrier(jnp.sum(offsets * weight[None], axis=3))

def accumulate(targets, operands):

    def add_tile(index, summed):
        sources = lax.dynamic_index_in_dim(operands, index, 1, keepdims=False)
        return summed + pair_accel(targets, sources)
    return lax.fori_loop(0, operands.shape[1], add_tile, jnp.zeros(targets.shape, targets.dtype))

def gather_pool(pool_rows, list_rows):
    return jnp.take(pool_rows, list_rows, axis=1)

def reference(positions, velocities, masses, long_kick, leaf_lists, ghost_ids, leaf_counts):
    places = jnp.moveaxis(positions.reshape(3, SLABS, COLUMNS, LEAVES, LEAF), 0, 2)
    speeds = jnp.moveaxis(velocities.reshape(3, SLABS, COLUMNS, LEAVES, LEAF), 0, 2)
    kicks = jnp.moveaxis(long_kick.reshape(3, SLABS, COLUMNS, LEAVES, LEAF), 0, 2)
    mass_rows = masses.reshape(SLABS, COLUMNS, 1, LEAVES, LEAF)
    lists = jnp.moveaxis(leaf_lists.reshape(NEIGHBOURS, SLABS, COLUMNS, LEAVES), 0, 2)
    ghosts = ghost_ids.reshape(SLABS, COLUMNS, 1, GHOSTS, 1)
    ghosts = jnp.broadcast_to(ghosts, (SLABS, COLUMNS, 4, GHOSTS, LEAF))
    counts = leaf_counts.reshape(SLABS, COLUMNS, 1, 1, 1)
    live = jnp.arange(LEAVES).astype(jnp.int32)[None, None, None, :, None] < counts
    for subcycle in range(SUBCYCLES):
        own_rows = jnp.concatenate([places, mass_rows], axis=2)
        chosen = jnp.take_along_axis(own_rows, ghosts, axis=3)
        parts = [own_rows]
        for shift_x in (-1, 0, 1):
            for shift_y in (-1, 0, 1):
                parts.append(jnp.roll(jnp.roll(chosen, -shift_x, axis=0), -shift_y, axis=1))
        pool = jnp.concatenate(parts, axis=3)
        operands = jax.vmap(jax.vmap(gather_pool))(pool, lists)

        def slab_accel(items):
            return jax.vmap(accumulate)(items[0], items[1])
        accel = lax.map(slab_accel, (places, operands))
        speeds = jnp.where(live, speeds + time_step * (accel + kicks), speeds)
        places = jnp.where(live, places + time_step * speeds, places)
    new_positions = jnp.moveaxis(places, 2, 0).reshape(3, -1)
    new_velocities = jnp.moveaxis(speeds, 2, 0).reshape(3, -1)
    return (new_positions, new_velocities)
```

```python
import functools

import jax
import jax.numpy as jnp
from jax import lax
from jax.experimental import pallas as pl
from jax.experimental.pallas import tpu as pltpu
from jax.sharding import PartitionSpec as P

SUBCYCLES = 4

soften_sq = 0.04
cutoff_sq = 9.0
time_step = 0.5

MESH = pl.DeviceIdType.MESH
PAIR_ROWS = 32
SUM_ROWS = 16
ROWS = PAIR_ROWS + SUM_ROWS
WAYS = [(a, b) for a in (-1, 0, 1) for b in (-1, 0, 1)]
BESIDE = [way for way in WAYS if way != (0, 0)]
LOW_PART = True
UNROLL = 2


def thirds(value):
    first = value.astype(jnp.bfloat16).astype(jnp.float32)
    rest = value - first
    second = rest.astype(jnp.bfloat16).astype(jnp.float32)
    return first, second, rest - second


def slot_of(a, b):
    return (a + 1) * 3 + b + 1


def kernel(
    sizes, p_in, v_in, mass, kick, live_in, lists, ghosts, p, v,
    wide, pool, targets, turned, sums, ghost_sums, ghost_v, ghost_kick, sent, got, send_sem, recv_sem,
):
    nx, ny = sizes
    leaves, lanes = mass.shape
    entries = lists.shape[0]
    lent = ghosts.shape[0]
    slots = wide.shape[0] // ROWS
    me_x, me_y = lax.axis_index("gx"), lax.axis_index("gy")

    def device(a, b):
        return (lax.rem(me_x + (a + nx), nx), lax.rem(me_y + (b + ny), ny))

    barrier = pltpu.get_barrier_semaphore()
    for a, b in BESIDE:
        pl.semaphore_signal(barrier, inc=1, device_id=device(a, b), device_id_type=MESH)

    p[...] = p_in[...]
    v[...] = v_in[...]
    for g in range(lent):
        leaf = ghosts[g]
        for c in range(3):
            sent[0, c, g] = p_in[c, leaf]
            ghost_v[c, g] = v_in[c, leaf]
            ghost_kick[c, g] = kick[c, leaf]
        row = mass[leaf]
        for k in range(SUBCYCLES):
            sent[k, 3, g] = row

    def copies(k):
        made = []
        for a, b in BESIDE:
            made.append(
                pltpu.make_async_remote_copy(
                    src_ref=sent.at[k],
                    dst_ref=got.at[k, slot_of(-a, -b)],
                    send_sem=send_sem.at[k, slot_of(a, b)],
                    recv_sem=recv_sem.at[k, slot_of(-a, -b)],
                    device_id=device(a, b),
                    device_id_type=MESH,
                )
            )
        return made

    flying = []
    pl.semaphore_wait(barrier, len(BESIDE))
    flying.append(copies(0))
    for copy in flying[0]:
        copy.start()

    def put(ref, height, base, total, row, value):
        ref[pl.ds(base * height + row, total, stride=height), :] = value

    ones = jnp.ones((slots, lanes), jnp.float32)
    zeros = jnp.zeros((slots, lanes), jnp.float32)
    for row in range(18, 21):
        put(targets, PAIR_ROWS, 0, leaves, row, ones[:leaves])
    for row in range(21, 24):
        put(wide, ROWS, 0, slots, row, ones)
    for row in range(24, PAIR_ROWS):
        put(wide, ROWS, 0, slots, row, zeros)
        put(targets, PAIR_ROWS, 0, leaves, row, zeros[:leaves])
    for row in range(PAIR_ROWS + 12, ROWS):
        put(wide, ROWS, 0, slots, row, zeros)

    def lay_out(base, total, place, weight):
        norm = None
        splits = []
        for c in range(3):
            scaled = place[c] * (cutoff_sq**-0.5)
            square = scaled * scaled
            norm = square if norm is None else norm + square
            one, two, three = thirds(scaled)
            splits.append((one, two, three))
            for row, value in enumerate((one, two, one, three, one, two)):
                put(wide, ROWS, base, total, c * 6 + row, value)
        for row, value in enumerate(thirds(-norm)):
            put(wide, ROWS, base, total, 18 + row, value)
        scaled_weight = weight * (cutoff_sq**-1.5)
        moments = [scaled_weight] + [scaled_weight * place[c] for c in range(3)]
        for c, moment in enumerate(moments):
            for row, value in enumerate(thirds(moment)):
                put(wide, ROWS, base, total, PAIR_ROWS + c * 3 + row, value)
        return splits, norm

    def leaf_sums(leaf, out, where):
        target = turned[leaf]
        total = jnp.zeros((lanes, SUM_ROWS), jnp.float32)
        for j in range(0, entries, 2):
            tiles = [pool[lists[e, leaf]] for e in range(j, min(j + 2, entries))]
            near = jnp.concatenate([tile[:PAIR_ROWS] for tile in tiles], axis=1)
            carry = jnp.concatenate([tile[PAIR_ROWS:] for tile in tiles], axis=1)
            inside = jnp.dot(target, near, preferred_element_type=jnp.float32)
            apart = jnp.maximum(
                (1.0 + soften_sq / cutoff_sq) - inside, soften_sq / cutoff_sq
            )
            inverse = lax.rsqrt(apart)
            taper = jnp.maximum(inside, 0.0) * inverse
            weight = taper * taper * inverse
            high = weight.astype(jnp.bfloat16)
            contract = (((1,), (1,)), ((), ()))
            total += lax.dot_general(high, carry, contract, preferred_element_type=jnp.float32)
            if LOW_PART:
                low = (weight - high.astype(jnp.float32)).astype(jnp.bfloat16)
                total += lax.dot_general(low, carry, contract, preferred_element_type=jnp.float32)
        out[pl.ds(pl.multiple_of(where * SUM_ROWS, SUM_ROWS), SUM_ROWS), :] = total.T

    def gathered(ref, total):
        parts = []
        for c in range(4):
            rows = [ref[pl.ds(c * 3 + r, total, stride=SUM_ROWS), :] for r in range(3)]
            parts.append(rows[0] + (rows[1] + rows[2]))
        return parts

    live = time_step * live_in[...]

    for k in range(SUBCYCLES):
        splits, norm = lay_out(0, leaves, [p[c] for c in range(3)], mass[...])
        for c in range(3):
            one, two, three = [2.0 * part for part in splits[c]]
            for row, value in enumerate((one, one, two, one, three, two)):
                put(targets, PAIR_ROWS, 0, leaves, c * 6 + row, value)
        for row, value in enumerate(thirds(1.0 - norm)):
            put(targets, PAIR_ROWS, 0, leaves, 21 + row, value)
        lay_out(
            leaves + slot_of(0, 0) * lent, lent, [sent[k, c] for c in range(3)], sent[k, 3]
        )
        for copy in flying[k]:
            copy.wait_recv()
        for a, b in BESIDE:
            at = slot_of(a, b)
            lay_out(leaves + at * lent, lent, [got[k, at, c] for c in range(3)], got[k, at, 3])

        step = 8

        def narrow(i, carry):
            rows = pl.ds(pl.multiple_of(i * (step * ROWS), step * ROWS), step * ROWS)
            tiles = wide[rows, :].astype(jnp.bfloat16).reshape(step, ROWS, lanes)
            pool[pl.ds(i * step, step)] = tiles
            return carry

        lax.fori_loop(0, slots // step, narrow, 0)

        def turn(i, carry):
            for u in range(4):
                leaf = i * 4 + u
                rows = pl.ds(pl.multiple_of(leaf * PAIR_ROWS, PAIR_ROWS), PAIR_ROWS)
                turned[leaf] = targets[rows, :].T.astype(jnp.bfloat16)
            return carry

        lax.fori_loop(0, leaves // 4, turn, 0)

        if k + 1 < SUBCYCLES:

            def lend(i, carry):
                for u in range(UNROLL):
                    g = i * UNROLL + u
                    leaf_sums(ghosts[g], ghost_sums, g)
                return carry

            lax.fori_loop(0, lent // UNROLL, lend, 0)
            total, *moments = gathered(ghost_sums, lent)
            for c in range(3):
                place = sent[k, c]
                accel = moments[c] - total * place
                speed = ghost_v[c] + time_step * (accel + ghost_kick[c])
                ghost_v[c] = speed
                sent[k + 1, c] = place + time_step * speed
            flying.append(copies(k + 1))
            for copy in flying[k + 1]:
                copy.start()

        def pull(i, carry):
            for u in range(UNROLL):
                leaf = i * UNROLL + u
                leaf_sums(leaf, sums, leaf)
            return carry

        lax.fori_loop(0, leaves // UNROLL, pull, 0)
        total, *moments = gathered(sums, leaves)
        for c in range(3):
            place, speed = p[c], v[c]
            accel = moments[c] - total * place
            faster = speed + live * (accel + kick[c])
            v[c] = faster
            p[c] = place + live * faster

    for made in flying:
        for copy in made:
            copy.wait_send()


def solution(mesh):
    sizes = (mesh.shape["gx"], mesh.shape["gy"])

    def body(positions, velocities, masses, long_kick, leaf_lists, ghost_ids, leaf_counts):
        leaves = leaf_lists.shape[1]
        lanes = masses.shape[0] // leaves
        lent = ghost_ids.shape[0]
        slots = leaves + len(WAYS) * lent
        state = jax.ShapeDtypeStruct((3, leaves, lanes), jnp.float32)
        live = (jnp.arange(leaves)[:, None] < leaf_counts).astype(jnp.float32)
        live = jnp.broadcast_to(live, (leaves, lanes))
        vmem = pl.BlockSpec(memory_space=pltpu.VMEM)
        smem = pl.BlockSpec(memory_space=pltpu.SMEM)
        f32 = jnp.float32
        places, speeds = pl.pallas_call(
            functools.partial(kernel, sizes),
            out_shape=(state, state),
            in_specs=[vmem] * 5 + [smem] * 2,
            out_specs=(vmem, vmem),
            scratch_shapes=[
                pltpu.VMEM((slots * ROWS, lanes), f32),
                pltpu.VMEM((slots, ROWS, lanes), jnp.bfloat16),
                pltpu.VMEM((leaves * PAIR_ROWS, lanes), f32),
                pltpu.VMEM((leaves, lanes, PAIR_ROWS), jnp.bfloat16),
                pltpu.VMEM((leaves * SUM_ROWS, lanes), f32),
                pltpu.VMEM((lent * SUM_ROWS, lanes), f32),
                pltpu.VMEM((3, lent, lanes), f32),
                pltpu.VMEM((3, lent, lanes), f32),
                pltpu.VMEM((SUBCYCLES, 4, lent, lanes), f32),
                pltpu.VMEM((SUBCYCLES, len(WAYS), 4, lent, lanes), f32),
                pltpu.SemaphoreType.DMA((SUBCYCLES, len(WAYS))),
                pltpu.SemaphoreType.DMA((SUBCYCLES, len(WAYS))),
            ],
            compiler_params=pltpu.CompilerParams(collective_id=0, has_side_effects=True),
        )(
            positions.reshape(3, leaves, lanes),
            velocities.reshape(3, leaves, lanes),
            masses.reshape(leaves, lanes),
            long_kick.reshape(3, leaves, lanes),
            live,
            leaf_lists,
            ghost_ids,
        )
        return places.reshape(3, -1), speeds.reshape(3, -1)

    return jax.shard_map(
        body,
        mesh=mesh,
        in_specs=(
            P(None, ("gx", "gy")),
            P(None, ("gx", "gy")),
            P(("gx", "gy")),
            P(None, ("gx", "gy")),
            P(None, ("gx", "gy")),
            P(("gx", "gy")),
            P(("gx", "gy")),
        ),
        out_specs=(P(None, ("gx", "gy")), P(None, ("gx", "gy"))),
        check_vma=False,
    )
```

```python
import functools

import jax
import jax.numpy as jnp
from jax import lax
from jax.experimental import pallas as pl
from jax.experimental.pallas import tpu as pltpu
from jax.sharding import PartitionSpec as P

SUBCYCLES = 4

soften_sq = 0.04
cutoff_sq = 9.0
time_step = 0.5

MESH = pl.DeviceIdType.MESH
PAIR_ROWS = 32
SUM_ROWS = 16
ROWS = PAIR_ROWS + SUM_ROWS
WAYS = [(a, b) for a in (-1, 0, 1) for b in (-1, 0, 1)]
BESIDE = [way for way in WAYS if way != (0, 0)]
LOW_PART = True
UNROLL = 4


def thirds(value):
    first = value.astype(jnp.bfloat16).astype(jnp.float32)
    rest = value - first
    second = rest.astype(jnp.bfloat16).astype(jnp.float32)
    return first, second, rest - second


def slot_of(a, b):
    return (a + 1) * 3 + b + 1


def kernel(
    sizes, p_in, v_in, mass, kick, live_in, lists, ghosts, p, v,
    wide, pool, targets, turned, sums, ghost_sums, ghost_v, ghost_kick, sent, got, send_sem, recv_sem,
):
    nx, ny = sizes
    leaves, lanes = mass.shape
    entries = lists.shape[0]
    lent = ghosts.shape[0]
    slots = wide.shape[0] // ROWS
    me_x, me_y = lax.axis_index("gx"), lax.axis_index("gy")

    def device(a, b):
        return (lax.rem(me_x + (a + nx), nx), lax.rem(me_y + (b + ny), ny))

    barrier = pltpu.get_barrier_semaphore()
    for a, b in BESIDE:
        pl.semaphore_signal(barrier, inc=1, device_id=device(a, b), device_id_type=MESH)

    p[...] = p_in[...]
    v[...] = v_in[...]
    for g in range(lent):
        leaf = ghosts[g]
        for c in range(3):
            sent[0, c, g] = p_in[c, leaf]
            ghost_v[c, g] = v_in[c, leaf]
            ghost_kick[c, g] = kick[c, leaf]
        row = mass[leaf]
        for k in range(SUBCYCLES):
            sent[k, 3, g] = row

    def copies(k):
        made = []
        for a, b in BESIDE:
            made.append(
                pltpu.make_async_remote_copy(
                    src_ref=sent.at[k],
                    dst_ref=got.at[k, slot_of(-a, -b)],
                    send_sem=send_sem.at[k, slot_of(a, b)],
                    recv_sem=recv_sem.at[k, slot_of(-a, -b)],
                    device_id=device(a, b),
                    device_id_type=MESH,
                )
            )
        return made

    flying = []
    pl.semaphore_wait(barrier, len(BESIDE))
    flying.append(copies(0))
    for copy in flying[0]:
        copy.start()

    def put(ref, height, base, total, row, value):
        ref[pl.ds(base * height + row, total, stride=height), :] = value

    ones = jnp.ones((slots, lanes), jnp.float32)
    zeros = jnp.zeros((slots, lanes), jnp.float32)
    for row in range(18, 21):
        put(targets, PAIR_ROWS, 0, leaves, row, ones[:leaves])
    for row in range(21, 24):
        put(wide, ROWS, 0, slots, row, ones)
    for row in range(24, PAIR_ROWS):
        put(wide, ROWS, 0, slots, row, zeros)
        put(targets, PAIR_ROWS, 0, leaves, row, zeros[:leaves])
    for row in range(PAIR_ROWS + 12, ROWS):
        put(wide, ROWS, 0, slots, row, zeros)

    def lay_out(base, total, place, weight):
        norm = None
        splits = []
        for c in range(3):
            scaled = place[c] * (cutoff_sq**-0.5)
            square = scaled * scaled
            norm = square if norm is None else norm + square
            one, two, three = thirds(scaled)
            splits.append((one, two, three))
            for row, value in enumerate((one, two, one, three, one, two)):
                put(wide, ROWS, base, total, c * 6 + row, value)
        for row, value in enumerate(thirds(-norm)):
            put(wide, ROWS, base, total, 18 + row, value)
        scaled_weight = weight * (cutoff_sq**-1.5)
        moments = [scaled_weight] + [scaled_weight * place[c] for c in range(3)]
        for c, moment in enumerate(moments):
            for row, value in enumerate(thirds(moment)):
                put(wide, ROWS, base, total, PAIR_ROWS + c * 3 + row, value)
        return splits, norm

    def leaf_sums(leaf, out, where):
        target = turned[leaf]
        total = jnp.zeros((lanes, SUM_ROWS), jnp.float32)
        for j in range(0, entries, 2):
            tiles = [pool[lists[e, leaf]] for e in range(j, min(j + 2, entries))]
            near = jnp.concatenate([tile[:PAIR_ROWS] for tile in tiles], axis=1)
            carry = jnp.concatenate([tile[PAIR_ROWS:] for tile in tiles], axis=1)
            inside = jnp.dot(target, near, preferred_element_type=jnp.float32)
            apart = jnp.maximum(
                (1.0 + soften_sq / cutoff_sq) - inside, soften_sq / cutoff_sq
            )
            inverse = lax.rsqrt(apart)
            taper = jnp.maximum(inside, 0.0) * inverse
            weight = taper * taper * inverse
            high = weight.astype(jnp.bfloat16)
            contract = (((1,), (1,)), ((), ()))
            total += lax.dot_general(high, carry, contract, preferred_element_type=jnp.float32)
            if LOW_PART:
                low = (weight - high.astype(jnp.float32)).astype(jnp.bfloat16)
                total += lax.dot_general(low, carry, contract, preferred_element_type=jnp.float32)
        out[pl.ds(pl.multiple_of(where * SUM_ROWS, SUM_ROWS), SUM_ROWS), :] = total.T

    def gathered(ref, total):
        parts = []
        for c in range(4):
            rows = [ref[pl.ds(c * 3 + r, total, stride=SUM_ROWS), :] for r in range(3)]
            parts.append(rows[0] + (rows[1] + rows[2]))
        return parts

    live = time_step * live_in[...]

    for k in range(SUBCYCLES):
        splits, norm = lay_out(0, leaves, [p[c] for c in range(3)], mass[...])
        for c in range(3):
            one, two, three = [2.0 * part for part in splits[c]]
            for row, value in enumerate((one, one, two, one, three, two)):
                put(targets, PAIR_ROWS, 0, leaves, c * 6 + row, value)
        for row, value in enumerate(thirds(1.0 - norm)):
            put(targets, PAIR_ROWS, 0, leaves, 21 + row, value)
        lay_out(
            leaves + slot_of(0, 0) * lent, lent, [sent[k, c] for c in range(3)], sent[k, 3]
        )
        for copy in flying[k]:
            copy.wait_recv()
        for a, b in BESIDE:
            at = slot_of(a, b)
            lay_out(leaves + at * lent, lent, [got[k, at, c] for c in range(3)], got[k, at, 3])

        step = 8

        def narrow(i, carry):
            rows = pl.ds(pl.multiple_of(i * (step * ROWS), step * ROWS), step * ROWS)
            tiles = wide[rows, :].astype(jnp.bfloat16).reshape(step, ROWS, lanes)
            pool[pl.ds(i * step, step)] = tiles
            return carry

        lax.fori_loop(0, slots // step, narrow, 0)

        def turn(i, carry):
            for u in range(4):
                leaf = i * 4 + u
                rows = pl.ds(pl.multiple_of(leaf * PAIR_ROWS, PAIR_ROWS), PAIR_ROWS)
                turned[leaf] = targets[rows, :].T.astype(jnp.bfloat16)
            return carry

        lax.fori_loop(0, leaves // 4, turn, 0)

        if k + 1 < SUBCYCLES:

            def lend(i, carry):
                for u in range(UNROLL):
                    g = i * UNROLL + u
                    leaf_sums(ghosts[g], ghost_sums, g)
                return carry

            lax.fori_loop(0, lent // UNROLL, lend, 0)
            total, *moments = gathered(ghost_sums, lent)
            for c in range(3):
                place = sent[k, c]
                accel = moments[c] - total * place
                speed = ghost_v[c] + time_step * (accel + ghost_kick[c])
                ghost_v[c] = speed
                sent[k + 1, c] = place + time_step * speed
            flying.append(copies(k + 1))
            for copy in flying[k + 1]:
                copy.start()

        def pull(i, carry):
            for u in range(UNROLL):
                leaf = i * UNROLL + u
                leaf_sums(leaf, sums, leaf)
            return carry

        lax.fori_loop(0, leaves // UNROLL, pull, 0)
        total, *moments = gathered(sums, leaves)
        for c in range(3):
            place, speed = p[c], v[c]
            accel = moments[c] - total * place
            faster = speed + live * (accel + kick[c])
            v[c] = faster
            p[c] = place + live * faster

    for made in flying:
        for copy in made:
            copy.wait_send()


def solution(mesh):
    sizes = (mesh.shape["gx"], mesh.shape["gy"])

    def body(positions, velocities, masses, long_kick, leaf_lists, ghost_ids, leaf_counts):
        leaves = leaf_lists.shape[1]
        lanes = masses.shape[0] // leaves
        lent = ghost_ids.shape[0]
        slots = leaves + len(WAYS) * lent
        state = jax.ShapeDtypeStruct((3, leaves, lanes), jnp.float32)
        live = (jnp.arange(leaves)[:, None] < leaf_counts).astype(jnp.float32)
        live = jnp.broadcast_to(live, (leaves, lanes))
        vmem = pl.BlockSpec(memory_space=pltpu.VMEM)
        smem = pl.BlockSpec(memory_space=pltpu.SMEM)
        f32 = jnp.float32
        places, speeds = pl.pallas_call(
            functools.partial(kernel, sizes),
            out_shape=(state, state),
            in_specs=[vmem] * 5 + [smem] * 2,
            out_specs=(vmem, vmem),
            scratch_shapes=[
                pltpu.VMEM((slots * ROWS, lanes), f32),
                pltpu.VMEM((slots, ROWS, lanes), jnp.bfloat16),
                pltpu.VMEM((leaves * PAIR_ROWS, lanes), f32),
                pltpu.VMEM((leaves, lanes, PAIR_ROWS), jnp.bfloat16),
                pltpu.VMEM((leaves * SUM_ROWS, lanes), f32),
                pltpu.VMEM((lent * SUM_ROWS, lanes), f32),
                pltpu.VMEM((3, lent, lanes), f32),
                pltpu.VMEM((3, lent, lanes), f32),
                pltpu.VMEM((SUBCYCLES, 4, lent, lanes), f32),
                pltpu.VMEM((SUBCYCLES, len(WAYS), 4, lent, lanes), f32),
                pltpu.SemaphoreType.DMA((SUBCYCLES, len(WAYS))),
                pltpu.SemaphoreType.DMA((SUBCYCLES, len(WAYS))),
            ],
            compiler_params=pltpu.CompilerParams(collective_id=0, has_side_effects=True),
        )(
            positions.reshape(3, leaves, lanes),
            velocities.reshape(3, leaves, lanes),
            masses.reshape(leaves, lanes),
            long_kick.reshape(3, leaves, lanes),
            live,
            leaf_lists,
            ghost_ids,
        )
        return places.reshape(3, -1), speeds.reshape(3, -1)

    return jax.shard_map(
        body,
        mesh=mesh,
        in_specs=(
            P(None, ("gx", "gy")),
            P(None, ("gx", "gy")),
            P(("gx", "gy")),
            P(None, ("gx", "gy")),
            P(None, ("gx", "gy")),
            P(("gx", "gy")),
            P(("gx", "gy")),
        ),
        out_specs=(P(None, ("gx", "gy")), P(None, ("gx", "gy"))),
        check_vma=False,
    )
```
